32 devices in a mesh: rep: 2 (over x), mp: 16 (over z, y, core).
Axes of the slice: x: 2, y: 2, z: 4, core: 2. Of those that a mesh axis runs over, the one named last changes fastest.
Arguments:
- tokens: bfloat16 [1280, 3072], P(('rep', 'mp')), may hold values from -6 to 6
- w_in: bfloat16 [2, 3072, 2, 12288], P('rep', None, None, 'mp'), may hold values from -0.109375 to 0.109375
- w_down: bfloat16 [2, 12288, 3072], P('rep', 'mp'), may hold values from -0.0546875 to 0.0546875
- norm_gain: float32 [3072], replicated, may hold values from 0.1 to 1.9
- final_gain: float32 [3072], replicated, may hold values from 0.1 to 1.9
- value_head: float32 [3072], replicated, may hold values from -0.6 to 0.6
- owner: int32 [16], P('mp'), may hold values from 0 to 1
- lengths: int32 [16], P('rep'), may hold values from 20 to 80, as said below
- offsets: int32 [16], P('rep'), may hold values from 0 to 620, as said below
Outputs:
- mixed: bfloat16 [1280, 3072], P(('rep', 'mp'))
- rewards: float32 [16], P('rep')
The draws below stay inside these ranges and needn't reach their ends.
Inputs may be any that keep to these rules, and one draw needn't show every extreme that they name: `lengths`: every rollout is at least a quarter of 80 long; in each group one rollout has exactly 80 tokens. `offsets`: rollout j of a group lies wholly within slots j * 80 to (j + 1) * 80 - 1 of its group; the other slots are padding.
All inputs are finite; a program needn't handle non-finite values.
Results may differ from the reference program's by a relative error of at most 0.0046.
Values may be sent and summed in bfloat16 or wider, within the bound.
A program may use at most 128 MiB of HBM per device.

```python
import jax
import jax.numpy as jnp
from jax import lax

D = 3072
FF = 12288
SEQ_GRP = 8
GROUP_TOK = 640
TOKENS = 1280
MAX_LEN = 80
SEQS = 16
N_REP = 2
N_MP = 16


def packed_layout(base):
    drawn = jax.random.randint(base, (N_REP, SEQ_GRP), MAX_LEN // 4, MAX_LEN + 1)
    longest = jax.random.randint(jax.random.fold_in(base, 1), (N_REP,), 0, SEQ_GRP)
    column = jnp.arange(SEQ_GRP, dtype=jnp.int32)
    drawn = jnp.where(column[None, :] == longest[:, None], MAX_LEN, drawn).astype(jnp.int32)
    spare = (MAX_LEN - drawn + 1).astype(jnp.int32)
    shift_bits = jax.random.randint(jax.random.fold_in(base, 2), (N_REP, SEQ_GRP), 0, 1 << 20)
    shift = (shift_bits % spare).astype(jnp.int32)
    starts = (column[None, :] * MAX_LEN + shift).astype(jnp.int32)
    return (drawn.reshape(-1), starts.reshape(-1))


def draw_lengths(key, part):
    return packed_layout(jax.random.fold_in(key, 7))[0]


def draw_offsets(key, part):
    return packed_layout(jax.random.fold_in(key, 7))[1]


def with_ends(array, key, smallest, top_value):
    place = [jax.random.randint(jax.random.fold_in(key, axis), (), 0, length) for axis, length in enumerate(array.shape)]
    main_axis = array.shape.index(max(array.shape))
    beside = place[:main_axis] + [(place[main_axis] + 1) % array.shape[main_axis]] + place[main_axis + 1:]
    return array.at[tuple(place)].set(smallest).at[tuple(beside)].set(top_value)


def block_scale(rng, shape, pieces, low, top_value):
    def one(position, parts):
        heights = jax.random.uniform(jax.random.fold_in(jax.random.fold_in(rng, 6), position), (parts,), jnp.float32, low / len(pieces), top_value / len(pieces))
        return jnp.repeat(jnp.exp(heights), shape[position] // parts).reshape((-1,) + (1,) * (len(shape) - position - 1))

    factor_of = one(*pieces[0])
    for cut in pieces[1:]:
        factor_of = factor_of * one(*cut)
    return factor_of


def bell_draw(key, shape, spread, bound, shards=(), held_as=jnp.bfloat16):
    loudness = block_scale(key, shape, shards, -0.22, 0.18) if shards else 1.0
    values = jax.random.normal(key, shape, jnp.float32) * spread * loudness
    return jnp.minimum(jnp.maximum(values, -bound), bound).astype(held_as)


def setup_inputs(seed: int = 0) -> dict:
    keys = jax.random.split(jax.random.key(seed), 10)
    tokens = bell_draw(keys[0], (TOKENS, D), 1.0, 6.0, ((0, 32),))
    w_in = bell_draw(keys[1], (N_REP, D, 2, FF), D ** -0.5, 0.109375, ((0, 2), (3, 16)))
    w_down = bell_draw(keys[2], (N_REP, FF, D), FF ** -0.5, 0.0546875, ((0, 2), (1, 16)))
    norm_gain = jnp.clip(1.0 + 0.18 * jax.random.normal(keys[3], (D,), jnp.float32), 0.1, 1.9)
    final_gain = jnp.clip(1.0 + 0.18 * jax.random.normal(keys[4], (D,), jnp.float32), 0.1, 1.9)
    value_head = bell_draw(keys[5], (D,), 0.1, 0.6, (), jnp.float32)
    owner = with_ends(jax.random.randint(keys[6], (N_MP,), 0, N_REP), jax.random.fold_in(keys[6], 1), 0, N_REP - 1).astype(jnp.int32)
    lengths = draw_lengths(jax.random.fold_in(keys[9], 71), 0)
    offsets = draw_offsets(jax.random.fold_in(keys[9], 71), 0)
    return dict(tokens=tokens, w_in=w_in, w_down=w_down, norm_gain=norm_gain, final_gain=final_gain, value_head=value_head, owner=owner, lengths=lengths, offsets=offsets)


def reference(tokens, w_in, w_down, norm_gain, final_gain, value_head, owner, lengths, offsets):
    shard_cols = FF // N_MP
    shard_ids = jnp.arange(N_MP, dtype=jnp.int32)
    inner_split = w_in.reshape(N_REP, D, 2, N_MP, shard_cols)
    inner_chosen = jnp.transpose(inner_split[owner, :, :, shard_ids, :], (1, 2, 0, 3)).reshape(D, 2, FF)
    gate_weight = inner_chosen[:, 0, :]
    up_weight = inner_chosen[:, 1, :]
    down_weight = w_down.reshape(N_REP, N_MP, shard_cols, D)[owner, shard_ids].reshape(FF, D)
    grouped = tokens.reshape(N_REP, GROUP_TOK, D)
    group_lengths = lengths.reshape(N_REP, SEQ_GRP)
    group_offsets = offsets.reshape(N_REP, SEQ_GRP)

    def one_group(packed):
        block, seq_lengths, seq_offsets = packed
        slots = jnp.arange(GROUP_TOK, dtype=jnp.int32)
        member = ((slots[:, None] >= seq_offsets[None, :]) & (slots[:, None] < seq_offsets[None, :] + seq_lengths[None, :])).astype(jnp.float32)
        live = lax.optimization_barrier(jnp.sum(member, axis=1))
        block_f = block.astype(jnp.float32)
        normed = (block_f * lax.rsqrt(lax.optimization_barrier(jnp.mean(block_f * block_f, axis=1, keepdims=True)) + 1e-06) * norm_gain).astype(jnp.bfloat16)
        gate_part = jnp.dot(normed, gate_weight, preferred_element_type=jnp.float32)
        up_part = jnp.dot(normed, up_weight, preferred_element_type=jnp.float32)
        hidden = (jax.nn.gelu(gate_part, approximate=True) * up_part * live[:, None]).astype(jnp.bfloat16)
        resid = block_f + jnp.dot(hidden, down_weight, preferred_element_type=jnp.float32)
        final = resid * lax.rsqrt(lax.optimization_barrier(jnp.mean(resid * resid, axis=1, keepdims=True)) + 1e-06) * final_gain
        values = jnp.dot(final, value_head, precision=lax.Precision.HIGHEST)
        totals = jnp.dot(values, member, precision=lax.Precision.HIGHEST)
        return (resid.astype(jnp.bfloat16), totals / seq_lengths.astype(jnp.float32))
    mixed, rewards = lax.map(one_group, (grouped, group_lengths, group_offsets))
    return (mixed.reshape(TOKENS, D), rewards.reshape(SEQS))
```

```python
import functools

import jax
import jax.numpy as jnp
from jax import lax
from jax.experimental import pallas as pl
from jax.experimental.pallas import tpu as pltpu
from jax.sharding import PartitionSpec as P


def spread(value, axis, source):
    kept = jnp.where(lax.axis_index(axis) == source, value, 0).astype(value.dtype)
    return lax.psum(kept, axis)


def membership(slots, lengths, offsets):
    inside = (slots[:, None] >= offsets[None, :]) & (
        slots[:, None] < offsets[None, :] + lengths[None, :]
    )
    return inside.astype(jnp.float32)


def norm_rows(tokens_f, norm_gain):
    return (
        tokens_f
        * lax.rsqrt(jnp.mean(tokens_f * tokens_f, axis=1, keepdims=True) + 1e-06)
        * norm_gain
    ).astype(jnp.bfloat16)


def finish(tokens_f, delta, final_gain, value_head, lengths, offsets):
    tok_rows = tokens_f.shape[0]
    resid = tokens_f + delta
    mixed = resid.astype(jnp.bfloat16)
    final = resid * lax.rsqrt(jnp.mean(resid * resid, axis=1, keepdims=True) + 1e-06) * final_gain
    values = jnp.dot(final, value_head, precision=lax.Precision.HIGHEST)
    own_slots = lax.axis_index("mp") * tok_rows + jnp.arange(tok_rows, dtype=jnp.int32)
    member = membership(own_slots, lengths, offsets)
    partial_sums = jnp.dot(values, member, precision=lax.Precision.HIGHEST)
    totals = lax.psum(partial_sums, "mp")
    rewards = totals / lengths.astype(jnp.float32)
    return (mixed, rewards)


def move_weights(tokens, w_in, w_down, norm_gain, final_gain, value_head, owner, lengths, offsets):
    owner_index = owner[0]
    width = tokens.shape[1]
    hidden_cols = w_in.shape[3]
    tokens_f = tokens.astype(jnp.float32)
    normed = norm_rows(tokens_f, norm_gain)
    inner_local, outer_local = (
        spread(w_in, "rep", owner_index),
        spread(w_down, "rep", owner_index),
    )
    inner_matrix = inner_local.reshape(width, 2 * hidden_cols)
    piece = lax.all_gather(normed, "mp", axis=0, tiled=True)
    slots = jnp.arange(piece.shape[0], dtype=jnp.int32)
    row_count = piece.shape[0]
    products = jnp.dot(piece, inner_matrix, preferred_element_type=jnp.float32).reshape(
        row_count, 2, hidden_cols
    )
    gate_part = products[:, 0, :]
    up_part = products[:, 1, :]
    hidden = (
        jax.nn.gelu(gate_part, approximate=True)
        * up_part
        * jnp.sum(membership(slots, lengths, offsets), axis=1)[:, None]
    ).astype(jnp.bfloat16)
    outer_matrix = outer_local.reshape(hidden_cols, width)
    delta = lax.psum_scatter(
        jnp.dot(hidden, outer_matrix, preferred_element_type=jnp.float32),
        "mp",
        scatter_dimension=0,
        tiled=True,
    )
    return finish(tokens_f, delta, final_gain, value_head, lengths, offsets)


MESH = pl.DeviceIdType.MESH


def place(half):
    rep, slot = lax.axis_index("rep"), lax.axis_index("mp")
    side, row, level = slot % 2, (slot // 2) % 2, slot // 4
    other_rep, other_row = 1 - rep, 1 - row
    first = (rep * side + other_rep * (1 - side), row * (1 - side) + other_row * side)
    second = (rep * (1 - side) + other_rep * side, row * side + other_row * (1 - side))
    return rep, slot, side, level, (rep, row), first, second, (other_rep, other_row)


def remote(src, dst, send_sem, recv_sem, column, level, side):
    return pltpu.make_async_remote_copy(
        src_ref=src, dst_ref=dst, send_sem=send_sem, recv_sem=recv_sem,
        device_id=(column[0], level * 4 + column[1] * 2 + side), device_id_type=MESH,
    )


def gather_kernel(half, own_ref, out_ref, level_send, first_send, second_send, cross_send, pass_send, recv_sem, local_sem):
    rep, slot, side, level, here, first, second, cross = place(half)
    levels = half // 2

    barrier = pltpu.get_barrier_semaphore()

    def greet(column, at, plane):
        pl.semaphore_signal(
            barrier, inc=1, device_id=(column[0], at * 4 + column[1] * 2 + plane), device_id_type=MESH
        )

    greet(first, level, side)
    greet(second, level, side)
    greet(here, level, 1 - side)

    @pl.loop(1, levels)
    def _(d):
        greet(here, (level + d) % levels, side)

    pl.semaphore_wait(barrier, levels + 2)

    def index_of(column, at):
        return (column[0] * half + at * 2 + column[1]) * 2 + side

    mine = index_of(here, level)

    def from_level(d):
        return (level + levels - d) % levels

    def climb(d):
        return remote(own_ref, out_ref.at[mine], level_send.at[d], recv_sem.at[mine], here, (level + d) % levels, side)

    def move(src, index, sem, column):
        return remote(src, out_ref.at[index], sem, recv_sem.at[index], column, level, side)

    def hand(src, index):
        return remote(src, out_ref.at[index], pass_send.at[index], recv_sem.at[index], here, level, 1 - side)

    def arrive(index):
        pltpu.make_async_copy(own_ref, out_ref.at[index], recv_sem.at[index]).wait()

    move(own_ref, mine, first_send.at[0], first).start()

    @pl.loop(1, levels)
    def _(d):
        climb(d).start()

    move(own_ref, mine, second_send.at[0], second).start()
    hand(own_ref, mine).start()
    keep = pltpu.make_async_copy(own_ref, out_ref.at[mine], local_sem)
    keep.start()

    def relay(d):
        index = index_of(first, from_level(d))
        arrive(index)
        move(out_ref.at[index], index, cross_send.at[d], second).start()
        hand(out_ref.at[index], index).start()

    def settle(d):
        for column in (second, cross):
            index = index_of(column, from_level(d))
            arrive(index)
            hand(out_ref.at[index], index).start()

    relay(0)

    @pl.loop(1, levels)
    def _(d):
        index = index_of(here, from_level(d))
        arrive(index)
        move(out_ref.at[index], index, first_send.at[d], first).start()
        move(out_ref.at[index], index, second_send.at[d], second).start()
        hand(out_ref.at[index], index).start()
        relay(d)
        settle(d - 1)

    settle(levels - 1)

    @pl.loop(0, 2 * half)
    def _(i):
        arrive(2 * i + 1 - side)

    keep.wait()

    @pl.loop(1, levels)
    def _(d):
        climb(d).wait_send()

    @pl.loop(0, levels)
    def _(d):
        for sem in (first_send, second_send, cross_send):
            move(own_ref, mine, sem.at[d], first).wait_send()

    @pl.loop(0, 2 * half)
    def _(i):
        hand(own_ref, 2 * i + side).wait_send()


def gather_rows(own, half):
    dma = pltpu.SemaphoreType.DMA
    levels = half // 2
    return pl.pallas_call(
        functools.partial(gather_kernel, half),
        out_shape=jax.ShapeDtypeStruct((4 * half,) + own.shape, own.dtype),
        in_specs=[pl.BlockSpec(memory_space=pltpu.VMEM)],
        out_specs=pl.BlockSpec(memory_space=pl.ANY),
        scratch_shapes=[
            dma((levels,)), dma((levels,)), dma((levels,)), dma((levels,)),
            dma((4 * half,)), dma((4 * half,)), dma,
        ],
        compiler_params=pltpu.CompilerParams(collective_id=0, has_side_effects=True),
    )(own)


def reduce_kernel(half, part_ref, tok_ref, live_ref, member_ref, final_ref, head_ref, mixed_ref, totals_ref,
                  swap_buf, mine_buf, sum_buf, cross_buf, first_buf, second_buf, level_buf, acc, mean_buf, own_mean,
                  swap_send, swap_recv, local_sem, send_sem, cross_recv, first_recv, second_recv, level_recv,
                  mean_send, mean_recv):
    rep, slot, side, level, here, first, second, cross = place(half)
    levels, parts = half // 2, 2 * half
    barrier = pltpu.get_barrier_semaphore()
    pl.semaphore_signal(barrier, inc=1, device_id=(1 - rep, slot), device_id_type=MESH)

    @pl.loop(1, parts)
    def _(d):
        pl.semaphore_signal(barrier, inc=1, device_id=(rep, (slot + d) % parts), device_id_type=MESH)

    pl.semaphore_wait(barrier, parts)

    def target(column, d):
        return column[0] * half + ((level + d) % levels) * 2 + column[1]

    def swap(to):
        return remote(
            part_ref.at[2 * to + 1 - side], swap_buf.at[to], swap_send.at[to], swap_recv.at[to], here, level, 1 - side
        )

    def fetch(to):
        return pltpu.make_async_copy(part_ref.at[2 * to + side], mine_buf.at[to], local_sem.at[to])

    def send(to, buf, sem, slot_at, column, at):
        return remote(sum_buf.at[to], buf.at[slot_at], send_sem.at[to], sem.at[slot_at], column, at, side)

    def arrive(buf, sem, at):
        pltpu.make_async_copy(sum_buf.at[0], buf.at[at], sem.at[at]).wait()

    def both(to):
        fetch(to).wait()
        swap(to).wait_recv()
        return mine_buf[to].astype(jnp.float32) + swap_buf[to].astype(jnp.float32)

    def start(to):
        swap(to).start()
        fetch(to).start()

    @pl.loop(1, levels + 1)
    def _(d):
        start(target(cross, d))
        start(target(second, d))

    @pl.loop(1, levels + 1)
    def _(d):
        start(target(first, d))
        start(target(here, d))

    @pl.loop(1, levels + 1)
    def _(d):
        at = (level + d) % levels
        to = target(cross, d)
        sum_buf[to] = both(to).astype(jnp.bfloat16)
        send(to, cross_buf, cross_recv, at, second, level).start()
        to = target(second, d)
        sum_buf[to] = both(to).astype(jnp.bfloat16)
        send(to, second_buf, second_recv, at, second, level).start()

    @pl.loop(1, levels + 1)
    def _(d):
        at = (level + d) % levels
        to = target(first, d)
        mine = both(to)
        arrive(cross_buf, cross_recv, at)
        sum_buf[to] = (mine + cross_buf[at].astype(jnp.float32)).astype(jnp.bfloat16)
        send(to, first_buf, first_recv, at, first, level).start()

    def collect(d):
        at = (level + d) % levels
        mine = both(target(here, d))
        arrive(second_buf, second_recv, at)
        arrive(first_buf, first_recv, at)
        return mine + (second_buf[at].astype(jnp.float32) + first_buf[at].astype(jnp.float32))

    @pl.loop(1, levels)
    def _(d):
        to = target(here, d)
        sum_buf[to] = collect(d).astype(jnp.bfloat16)
        send(to, level_buf, level_recv, level, here, (level + d) % levels).start()

    acc[...] = collect(0)

    @pl.loop(1, levels)
    def _(d):
        at = (level + levels - d) % levels
        arrive(level_buf, level_recv, at)
        acc[...] += level_buf[at].astype(jnp.float32)

    resid = tok_ref[...].astype(jnp.float32) + acc[...] * live_ref[...]
    mixed_ref[...] = resid.astype(jnp.bfloat16)
    scale = lax.rsqrt(jnp.mean(resid * resid, axis=1, keepdims=True) + 1e-06)
    values = jnp.sum(resid * scale * final_ref[...] * head_ref[...], axis=1, keepdims=True)
    own_mean[...] = jnp.broadcast_to(jnp.sum(values * member_ref[...], axis=0, keepdims=True), own_mean.shape)

    def tell(d):
        to = (slot + d) % parts
        return pltpu.make_async_remote_copy(
            src_ref=own_mean, dst_ref=mean_buf.at[slot], send_sem=mean_send.at[to],
            recv_sem=mean_recv.at[slot], device_id=(rep, to), device_id_type=MESH,
        )

    @pl.loop(1, parts)
    def _(d):
        tell(d).start()

    totals_ref[...] = own_mean[...]

    @pl.loop(1, parts)
    def _(d):
        index = (slot + parts - d) % parts
        pltpu.make_async_copy(own_mean, mean_buf.at[index], mean_recv.at[index]).wait()
        totals_ref[...] += mean_buf[index]

    @pl.loop(0, levels)
    def _(d):
        for column in (cross, second, first, here):
            swap(target(column, d)).wait_send()
        for column in (cross, second, first):
            send(target(column, d), cross_buf, cross_recv, level, second, level).wait_send()

    @pl.loop(1, levels)
    def _(d):
        send(target(here, d), level_buf, level_recv, level, second, level).wait_send()

    @pl.loop(1, parts)
    def _(d):
        tell(d).wait_send()


def reduce_rows(part, tokens, live, member, final_gain, value_head, half):
    shape = tokens.shape
    levels, chips, parts = half // 2, 2 * half, 2 * half
    vmem = pl.BlockSpec(memory_space=pltpu.VMEM)
    dma = pltpu.SemaphoreType.DMA
    block = pltpu.VMEM((chips,) + shape, jnp.bfloat16)
    few = pltpu.VMEM((levels,) + shape, jnp.bfloat16)
    return pl.pallas_call(
        functools.partial(reduce_kernel, half),
        out_shape=(
            jax.ShapeDtypeStruct(shape, jnp.bfloat16),
            jax.ShapeDtypeStruct((8, 128), jnp.float32),
        ),
        in_specs=[pl.BlockSpec(memory_space=pl.ANY)] + [vmem] * 5,
        out_specs=(vmem, vmem),
        scratch_shapes=[
            block, block, block, few, few, few, few,
            pltpu.VMEM(shape, jnp.float32),
            pltpu.VMEM((parts, 8, 128), jnp.float32),
            pltpu.VMEM((8, 128), jnp.float32),
            dma((chips,)), dma((chips,)), dma((chips,)), dma((chips,)),
            dma((levels,)), dma((levels,)), dma((levels,)), dma((levels,)),
            dma((parts,)), dma((parts,)),
        ],
        compiler_params=pltpu.CompilerParams(
            collective_id=1, has_side_effects=True, vmem_limit_bytes=48 << 20
        ),
    )(part, tokens, live, member, final_gain[None, :], value_head[None, :])


def move_rows(reps, parts, tokens, w_in, w_down, norm_gain, final_gain, value_head, owner, lengths, offsets):
    tok_rows, width = tokens.shape
    half = parts // 2
    normed = norm_rows(tokens.astype(jnp.float32), norm_gain)
    rows = gather_rows(normed, half).reshape(reps * parts * tok_rows, width)
    gate = jnp.dot(rows, w_in[0, :, 0, :], preferred_element_type=jnp.float32)
    up = jnp.dot(rows, w_in[0, :, 1, :], preferred_element_type=jnp.float32)
    mine = owner[0] == lax.axis_index("rep")
    hidden = jnp.where(mine, jax.nn.gelu(gate, approximate=True) * up, 0.0).astype(jnp.bfloat16)
    part = jnp.dot(hidden, w_down[0], preferred_element_type=jnp.float32).astype(jnp.bfloat16)
    own_slots = lax.axis_index("mp") * tok_rows + jnp.arange(tok_rows, dtype=jnp.int32)
    member = membership(own_slots, lengths, offsets)
    live = jnp.sum(member, axis=1)[:, None]
    count = lengths.shape[0]
    member = jnp.pad(member, ((0, 0), (0, 128 - count)))
    mixed, totals = reduce_rows(
        part.reshape(reps * parts, tok_rows, width), tokens, live, member, final_gain, value_head, half
    )
    return mixed, totals[0, :count] / lengths.astype(jnp.float32)


def lengths_fit(args):
    return args[7].shape[0] <= 128


def per_device(reps, parts, *args):
    tokens, w_in, w_down = args[:3]
    row_bytes = 2 * reps * parts * tokens.size * 2
    weight_bytes = 2 * (w_in.size + w_down.size)
    if reps == 2 and parts % 4 == 0 and lengths_fit(args) and row_bytes < 2 * weight_bytes:
        return move_rows(reps, parts, *args)
    return move_weights(*args)


def solution(mesh):
    in_specs = (
        P(("rep", "mp"), None),
        P("rep", None, None, "mp"),
        P("rep", "mp", None),
        P(),
        P(),
        P(),
        P("mp"),
        P("rep"),
        P("rep"),
    )
    out_specs = (P(("rep", "mp"), None), P("rep"))
    return jax.shard_map(
        functools.partial(per_device, mesh.shape["rep"], mesh.shape["mp"]),
        mesh=mesh, in_specs=in_specs, out_specs=out_specs, check_vma=False,
    )
```

```python
import functools

import jax
import jax.numpy as jnp
from jax import lax
from jax.experimental import pallas as pl
from jax.experimental.pallas import tpu as pltpu
from jax.sharding import PartitionSpec as P


def spread(value, axis, source):
    kept = jnp.where(lax.axis_index(axis) == source, value, 0).astype(value.dtype)
    return lax.psum(kept, axis)


def membership(slots, lengths, offsets):
    inside = (slots[:, None] >= offsets[None, :]) & (
        slots[:, None] < offsets[None, :] + lengths[None, :]
    )
    return inside.astype(jnp.float32)


def norm_rows(tokens_f, norm_gain):
    return (
        tokens_f
        * lax.rsqrt(jnp.mean(tokens_f * tokens_f, axis=1, keepdims=True) + 1e-06)
        * norm_gain
    ).astype(jnp.bfloat16)


def finish(tokens_f, delta, final_gain, value_head, lengths, offsets):
    tok_rows = tokens_f.shape[0]
    resid = tokens_f + delta
    mixed = resid.astype(jnp.bfloat16)
    final = resid * lax.rsqrt(jnp.mean(resid * resid, axis=1, keepdims=True) + 1e-06) * final_gain
    values = jnp.dot(final, value_head, precision=lax.Precision.HIGHEST)
    own_slots = lax.axis_index("mp") * tok_rows + jnp.arange(tok_rows, dtype=jnp.int32)
    member = membership(own_slots, lengths, offsets)
    partial_sums = jnp.dot(values, member, precision=lax.Precision.HIGHEST)
    totals = lax.psum(partial_sums, "mp")
    rewards = totals / lengths.astype(jnp.float32)
    return (mixed, rewards)


def move_weights(tokens, w_in, w_down, norm_gain, final_gain, value_head, owner, lengths, offsets):
    owner_index = owner[0]
    width = tokens.shape[1]
    hidden_cols = w_in.shape[3]
    tokens_f = tokens.astype(jnp.float32)
    normed = norm_rows(tokens_f, norm_gain)
    inner_local, outer_local = (
        spread(w_in, "rep", owner_index),
        spread(w_down, "rep", owner_index),
    )
    inner_matrix = inner_local.reshape(width, 2 * hidden_cols)
    piece = lax.all_gather(normed, "mp", axis=0, tiled=True)
    slots = jnp.arange(piece.shape[0], dtype=jnp.int32)
    row_count = piece.shape[0]
    products = jnp.dot(piece, inner_matrix, preferred_element_type=jnp.float32).reshape(
        row_count, 2, hidden_cols
    )
    gate_part = products[:, 0, :]
    up_part = products[:, 1, :]
    hidden = (
        jax.nn.gelu(gate_part, approximate=True)
        * up_part
        * jnp.sum(membership(slots, lengths, offsets), axis=1)[:, None]
    ).astype(jnp.bfloat16)
    outer_matrix = outer_local.reshape(hidden_cols, width)
    delta = lax.psum_scatter(
        jnp.dot(hidden, outer_matrix, preferred_element_type=jnp.float32),
        "mp",
        scatter_dimension=0,
        tiled=True,
    )
    return finish(tokens_f, delta, final_gain, value_head, lengths, offsets)


MESH = pl.DeviceIdType.MESH


def place(half):
    rep, slot = lax.axis_index("rep"), lax.axis_index("mp")
    side, row, level = slot % 2, (slot // 2) % 2, slot // 4
    other_rep, other_row = 1 - rep, 1 - row
    first = (rep * side + other_rep * (1 - side), row * (1 - side) + other_row * side)
    second = (rep * (1 - side) + other_rep * side, row * side + other_row * (1 - side))
    return rep, slot, side, level, (rep, row), first, second, (other_rep, other_row)


def remote(src, dst, send_sem, recv_sem, column, level, side):
    return pltpu.make_async_remote_copy(
        src_ref=src, dst_ref=dst, send_sem=send_sem, recv_sem=recv_sem,
        device_id=(column[0], level * 4 + column[1] * 2 + side), device_id_type=MESH,
    )


def gather_kernel(half, own_ref, out_ref, level_send, first_send, second_send, cross_send, pass_send, recv_sem, local_sem):
    rep, slot, side, level, here, first, second, cross = place(half)
    levels = half // 2

    barrier = pltpu.get_barrier_semaphore()

    def greet(column, at, plane):
        pl.semaphore_signal(
            barrier, inc=1, device_id=(column[0], at * 4 + column[1] * 2 + plane), device_id_type=MESH
        )

    greet(first, level, side)
    greet(second, level, side)
    greet(here, level, 1 - side)

    @pl.loop(1, levels)
    def _(d):
        greet(here, (level + d) % levels, side)

    pl.semaphore_wait(barrier, levels + 2)

    def index_of(column, at):
        return (column[0] * half + at * 2 + column[1]) * 2 + side

    mine = index_of(here, level)

    def from_level(d):
        return (level + levels - d) % levels

    def climb(d):
        return remote(own_ref, out_ref.at[mine], level_send.at[d], recv_sem.at[mine], here, (level + d) % levels, side)

    def move(src, index, sem, column):
        return remote(src, out_ref.at[index], sem, recv_sem.at[index], column, level, side)

    def hand(src, index):
        return remote(src, out_ref.at[index], pass_send.at[index], recv_sem.at[index], here, level, 1 - side)

    def arrive(index):
        pltpu.make_async_copy(own_ref, out_ref.at[index], recv_sem.at[index]).wait()

    move(own_ref, mine, first_send.at[0], first).start()

    @pl.loop(1, levels)
    def _(d):
        climb(d).start()

    move(own_ref, mine, second_send.at[0], second).start()
    hand(own_ref, mine).start()
    keep = pltpu.make_async_copy(own_ref, out_ref.at[mine], local_sem)
    keep.start()

    def relay(d):
        index = index_of(first, from_level(d))
        arrive(index)
        move(out_ref.at[index], index, cross_send.at[d], second).start()
        hand(out_ref.at[index], index).start()

    def settle(d):
        for column in (second, cross):
            index = index_of(column, from_level(d))
            arrive(index)
            hand(out_ref.at[index], index).start()

    relay(0)

    @pl.loop(1, levels)
    def _(d):
        index = index_of(here, from_level(d))
        arrive(index)
        move(out_ref.at[index], index, first_send.at[d], first).start()
        move(out_ref.at[index], index, second_send.at[d], second).start()
        hand(out_ref.at[index], index).start()
        relay(d)
        settle(d - 1)

    settle(levels - 1)

    @pl.loop(0, 2 * half)
    def _(i):
        arrive(2 * i + 1 - side)

    keep.wait()

    @pl.loop(1, levels)
    def _(d):
        climb(d).wait_send()

    @pl.loop(0, levels)
    def _(d):
        for sem in (first_send, second_send, cross_send):
            move(own_ref, mine, sem.at[d], first).wait_send()

    @pl.loop(0, 2 * half)
    def _(i):
        hand(own_ref, 2 * i + side).wait_send()


def gather_rows(own, half):
    dma = pltpu.SemaphoreType.DMA
    levels = half // 2
    return pl.pallas_call(
        functools.partial(gather_kernel, half),
        out_shape=jax.ShapeDtypeStruct((4 * half,) + own.shape, own.dtype),
        in_specs=[pl.BlockSpec(memory_space=pltpu.VMEM)],
        out_specs=pl.BlockSpec(memory_space=pl.ANY),
        scratch_shapes=[
            dma((levels,)), dma((levels,)), dma((levels,)), dma((levels,)),
            dma((4 * half,)), dma((4 * half,)), dma,
        ],
        compiler_params=pltpu.CompilerParams(collective_id=0, has_side_effects=True),
    )(own)


def reduce_kernel(half, part_ref, tok_ref, live_ref, member_ref, final_ref, head_ref, mixed_ref, totals_ref,
                  swap_buf, mine_buf, sum_buf, cross_buf, first_buf, second_buf, level_buf, acc, mean_buf, own_mean,
                  swap_send, swap_recv, local_sem, send_sem, cross_recv, first_recv, second_recv, level_recv,
                  mean_send, mean_recv):
    rep, slot, side, level, here, first, second, cross = place(half)
    levels, parts = half // 2, 2 * half
    barrier = pltpu.get_barrier_semaphore()
    pl.semaphore_signal(barrier, inc=1, device_id=(1 - rep, slot), device_id_type=MESH)

    @pl.loop(1, parts)
    def _(d):
        pl.semaphore_signal(barrier, inc=1, device_id=(rep, (slot + d) % parts), device_id_type=MESH)

    pl.semaphore_wait(barrier, parts)

    def target(column, d):
        return column[0] * half + ((level + d) % levels) * 2 + column[1]

    def swap(to):
        return remote(
            part_ref.at[2 * to + 1 - side], swap_buf.at[to], swap_send.at[to], swap_recv.at[to], here, level, 1 - side
        )

    def fetch(to):
        return pltpu.make_async_copy(part_ref.at[2 * to + side], mine_buf.at[to], local_sem.at[to])

    def send(to, buf, sem, slot_at, column, at):
        return remote(sum_buf.at[to], buf.at[slot_at], send_sem.at[to], sem.at[slot_at], column, at, side)

    def arrive(buf, sem, at):
        pltpu.make_async_copy(sum_buf.at[0], buf.at[at], sem.at[at]).wait()

    def both(to):
        fetch(to).wait()
        swap(to).wait_recv()
        return mine_buf[to].astype(jnp.float32) + swap_buf[to].astype(jnp.float32)

    def start(to):
        swap(to).start()
        fetch(to).start()

    @pl.loop(1, levels + 1)
    def _(d):
        start(target(cross, d))
        start(target(second, d))

    @pl.loop(1, levels + 1)
    def _(d):
        start(target(first, d))
        start(target(here, d))

    @pl.loop(1, levels + 1)
    def _(d):
        at = (level + d) % levels
        to = target(cross, d)
        sum_buf[to] = both(to).astype(jnp.bfloat16)
        send(to, cross_buf, cross_recv, at, second, level).start()
        to = target(second, d)
        sum_buf[to] = both(to).astype(jnp.bfloat16)
        send(to, second_buf, second_recv, at, second, level).start()

    @pl.loop(1, levels + 1)
    def _(d):
        at = (level + d) % levels
        to = target(first, d)
        mine = both(to)
        arrive(cross_buf, cross_recv, at)
        sum_buf[to] = (mine + cross_buf[at].astype(jnp.float32)).astype(jnp.bfloat16)
        send(to, first_buf, first_recv, at, first, level).start()

    def collect(d):
        at = (level + d) % levels
        mine = both(target(here, d))
        arrive(second_buf, second_recv, at)
        arrive(first_buf, first_recv, at)
        return mine + (second_buf[at].astype(jnp.float32) + first_buf[at].astype(jnp.float32))

    @pl.loop(1, levels)
    def _(d):
        to = target(here, d)
        sum_buf[to] = collect(d).astype(jnp.bfloat16)
        send(to, level_buf, level_recv, level, here, (level + d) % levels).start()

    acc[...] = collect(0)

    @pl.loop(1, levels)
    def _(d):
        at = (level + levels - d) % levels
        arrive(level_buf, level_recv, at)
        acc[...] += level_buf[at].astype(jnp.float32)

    resid = tok_ref[...].astype(jnp.float32) + acc[...] * live_ref[...]
    mixed_ref[...] = resid.astype(jnp.bfloat16)
    scale = lax.rsqrt(jnp.mean(resid * resid, axis=1, keepdims=True) + 1e-06)
    values = jnp.sum(resid * scale * final_ref[...] * head_ref[...], axis=1, keepdims=True)
    own_mean[...] = jnp.broadcast_to(jnp.sum(values * member_ref[...], axis=0, keepdims=True), own_mean.shape)

    def tell(d):
        to = (slot + d) % parts
        return pltpu.make_async_remote_copy(
            src_ref=own_mean, dst_ref=mean_buf.at[slot], send_sem=mean_send.at[to],
            recv_sem=mean_recv.at[slot], device_id=(rep, to), device_id_type=MESH,
        )

    @pl.loop(1, parts)
    def _(d):
        tell(d).start()

    totals_ref[...] = own_mean[...]

    @pl.loop(1, parts)
    def _(d):
        index = (slot + parts - d) % parts
        pltpu.make_async_copy(own_mean, mean_buf.at[index], mean_recv.at[index]).wait()
        totals_ref[...] += mean_buf[index]

    @pl.loop(0, levels)
    def _(d):
        for column in (cross, second, first, here):
            swap(target(column, d)).wait_send()
        for column in (cross, second, first):
            send(target(column, d), cross_buf, cross_recv, level, second, level).wait_send()

    @pl.loop(1, levels)
    def _(d):
        send(target(here, d), level_buf, level_recv, level, second, level).wait_send()

    @pl.loop(1, parts)
    def _(d):
        tell(d).wait_send()


def reduce_rows(part, tokens, live, member, final_gain, value_head, half):
    shape = tokens.shape
    levels, chips, parts = half // 2, 2 * half, 2 * half
    vmem = pl.BlockSpec(memory_space=pltpu.VMEM)
    dma = pltpu.SemaphoreType.DMA
    block = pltpu.VMEM((chips,) + shape, jnp.bfloat16)
    few = pltpu.VMEM((levels,) + shape, jnp.bfloat16)
    return pl.pallas_call(
        functools.partial(reduce_kernel, half),
        out_shape=(
            jax.ShapeDtypeStruct(shape, jnp.bfloat16),
            jax.ShapeDtypeStruct((8, 128), jnp.float32),
        ),
        in_specs=[pl.BlockSpec(memory_space=pl.ANY)] + [vmem] * 5,
        out_specs=(vmem, vmem),
        scratch_shapes=[
            block, block, block, few, few, few, few,
            pltpu.VMEM(shape, jnp.float32),
            pltpu.VMEM((parts, 8, 128), jnp.float32),
            pltpu.VMEM((8, 128), jnp.float32),
            dma((chips,)), dma((chips,)), dma((chips,)), dma((chips,)),
            dma((levels,)), dma((levels,)), dma((levels,)), dma((levels,)),
            dma((parts,)), dma((parts,)),
        ],
        compiler_params=pltpu.CompilerParams(
            collective_id=1, has_side_effects=True, vmem_limit_bytes=48 << 20
        ),
    )(part, tokens, live, member, final_gain[None, :], value_head[None, :])


def move_rows(reps, parts, tokens, w_in, w_down, norm_gain, final_gain, value_head, owner, lengths, offsets):
    tok_rows, width = tokens.shape
    half = parts // 2
    normed = norm_rows(tokens.astype(jnp.float32), norm_gain)
    rows = gather_rows(normed, half).reshape(reps * parts * tok_rows, width)
    cols = w_in.shape[3]
    products = jnp.dot(rows, w_in.reshape(width, 2 * cols), preferred_element_type=jnp.float32)
    gate, up = products[:, :cols], products[:, cols:]
    mine = owner[0] == lax.axis_index("rep")
    hidden = jnp.where(mine, jax.nn.gelu(gate, approximate=True) * up, 0.0).astype(jnp.bfloat16)
    hidden = lax.optimization_barrier(hidden)
    part = jnp.dot(hidden, w_down[0], preferred_element_type=jnp.float32).astype(jnp.bfloat16)
    own_slots = lax.axis_index("mp") * tok_rows + jnp.arange(tok_rows, dtype=jnp.int32)
    member = membership(own_slots, lengths, offsets)
    live = jnp.sum(member, axis=1)[:, None]
    count = lengths.shape[0]
    member = jnp.pad(member, ((0, 0), (0, 128 - count)))
    mixed, totals = reduce_rows(
        part.reshape(reps * parts, tok_rows, width), tokens, live, member, final_gain, value_head, half
    )
    return mixed, totals[0, :count] / lengths.astype(jnp.float32)


def lengths_fit(args):
    return args[7].shape[0] <= 128


def per_device(reps, parts, *args):
    tokens, w_in, w_down = args[:3]
    row_bytes = 2 * reps * parts * tokens.size * 2
    weight_bytes = 2 * (w_in.size + w_down.size)
    if reps == 2 and parts % 4 == 0 and lengths_fit(args) and row_bytes < 2 * weight_bytes:
        return move_rows(reps, parts, *args)
    return move_weights(*args)


def solution(mesh):
    in_specs = (
        P(("rep", "mp"), None),
        P("rep", None, None, "mp"),
        P("rep", "mp", None),
        P(),
        P(),
        P(),
        P("mp"),
        P("rep"),
        P("rep"),
    )
    out_specs = (P(("rep", "mp"), None), P("rep"))
    return jax.shard_map(
        functools.partial(per_device, mesh.shape["rep"], mesh.shape["mp"]),
        mesh=mesh, in_specs=in_specs, out_specs=out_specs, check_vma=False,
    )
```
